32 devices in a mesh: expert: 4 (over y, core), shard: 8 (over z, x).
Axes of the slice: x: 2, y: 2, z: 4, core: 2. Of those that a mesh axis runs over, the one named last changes fastest.
Arguments:
- master_gate: float32 [128, 2048, 768], P('expert', 'shard'), may hold values from -0.125 to 0.125
- second_gate: bfloat16 [128, 2048, 768], P('expert', 'shard'), may hold values from -0.0625 to 0.0625
- master_up: float32 [128, 2048, 768], P('expert', 'shard'), may hold values from -0.125 to 0.125
- second_up: bfloat16 [128, 2048, 768], P('expert', 'shard'), may hold values from -0.0625 to 0.0625
- router_weight: float32 [2048, 128], P('shard', 'expert'), may hold values from -0.125 to 0.125
- router_gain: float32 [2048], P('shard'), may hold values from 0.25 to 1.75
Outputs:
- final_gate: bfloat16 [128, 768, 2048], P('expert', 'shard')
- final_up: bfloat16 [128, 768, 2048], P('expert', 'shard')
- serve_router: bfloat16 [2048, 128], replicated
The draws below stay inside these ranges and needn't reach their ends.
All inputs are finite; a program needn't handle non-finite values.
Results may differ from the reference program's by a relative error of at most 0.001.
Values may be sent and summed in bfloat16 or wider, within the bound.
A program may use at most 192 MiB of HBM per device.

```python
import jax
import jax.numpy as jnp

EXPERTS = 128
D_MODEL = 2048
D_EXPERT = 768


def block_levels(own_key, shape, split, low, largest):
    factor_of = 1.0
    for position, parts in split:
        steps = jax.random.uniform(jax.random.fold_in(jax.random.fold_in(own_key, 6), position), (parts,), jnp.float32, low / len(split), largest / len(split))
        factor_of = factor_of * jnp.repeat(jnp.exp(steps), shape[position] // parts).reshape((-1,) + (1,) * (len(shape) - 1 - position))
    return factor_of


def scatter_about(stream_key, dims, width, bound, shards=(), dtype=jnp.bfloat16):
    entries = jax.random.normal(stream_key, dims, jnp.float32) * width
    if len(shards) > 0:
        entries = block_levels(stream_key, dims, shards, -0.22, 0.18) * entries
    return jnp.clip(entries, min=-bound, max=bound).astype(dtype)


def setup_inputs(seed: int = 0) -> dict:
    keys = jax.random.split(jax.random.key(seed), 7)
    master_gate = scatter_about(keys[0], (EXPERTS, D_MODEL, D_EXPERT), D_MODEL ** -0.5, 0.125, ((0, 4), (1, 8)), jnp.float32)
    second_gate = scatter_about(keys[1], (EXPERTS, D_MODEL, D_EXPERT), (D_MODEL * 4) ** -0.5, 0.0625, ((0, 4), (1, 8)))
    master_up = scatter_about(keys[2], (EXPERTS, D_MODEL, D_EXPERT), D_MODEL ** -0.5, 0.125, ((0, 4), (1, 8)), jnp.float32)
    second_up = scatter_about(keys[3], (EXPERTS, D_MODEL, D_EXPERT), (D_MODEL * 4) ** -0.5, 0.0625, ((0, 4), (1, 8)))
    router_weight = scatter_about(keys[4], (D_MODEL, EXPERTS), D_MODEL ** -0.5, 0.125, ((0, 8), (1, 4)), jnp.float32)
    router_gain = jnp.clip(1.0 + 0.15 * jax.random.normal(keys[5], (D_MODEL,), jnp.float32), 0.25, 1.75)
    return {"master_gate": master_gate, "second_gate": second_gate, "master_up": master_up, "second_up": second_up, "router_weight": router_weight, "router_gain": router_gain}


def reference(master_gate, second_gate, master_up, second_up, router_weight, router_gain):
    merged_gate = master_gate + second_gate.astype(jnp.float32)
    merged_up = master_up + second_up.astype(jnp.float32)
    final_gate = merged_gate.astype(jnp.bfloat16)
    final_gate = jnp.transpose(final_gate, (0, 2, 1))
    final_up = merged_up.astype(jnp.bfloat16)
    final_up = jnp.transpose(final_up, (0, 2, 1))
    serve_router = (router_weight * router_gain[:, None]).astype(jnp.bfloat16)
    return final_gate, final_up, serve_router
```

```python
import functools

import jax
import jax.numpy as jnp
from jax import lax
from jax.experimental import pallas as pl
from jax.experimental.pallas import tpu as pltpu
from jax.sharding import PartitionSpec as P

MESH = pl.DeviceIdType.MESH
SLOTS = 3
ORDER = 0


def exchange_kernel(
    n, groups, mg, sg, mu, su, part, recv, router,
    wide, narrow, outbox, in_sem, send_sem, recv_sem, own_sem, rs_send, rs_recv, re_send, re_recv,
):
    experts, rows, _ = mg.shape
    block = outbox.shape[3]
    columns = part.shape[0]
    me = lax.axis_index("shard")
    group = lax.axis_index("expert")

    def load(e):
        slot = lax.rem(e, SLOTS)
        return (
            pltpu.make_async_copy(mg.at[e], wide.at[slot, 0], in_sem.at[slot, 0]),
            pltpu.make_async_copy(sg.at[e], narrow.at[slot, 0], in_sem.at[slot, 1]),
            pltpu.make_async_copy(mu.at[e], wide.at[slot, 1], in_sem.at[slot, 2]),
            pltpu.make_async_copy(su.at[e], narrow.at[slot, 1], in_sem.at[slot, 3]),
        )

    for e in range(SLOTS):
        for copy in load(e):
            copy.start()

    barrier = pltpu.get_barrier_semaphore()
    for j in range(1, n):
        pl.semaphore_signal(barrier, inc=1, device_id=(group, lax.rem(me + j, n)), device_id_type=MESH)
    for j in range(1, groups):
        pl.semaphore_signal(barrier, inc=1, device_id=(lax.rem(group + j, groups), me), device_id_type=MESH)
    pl.semaphore_wait(barrier, n - 1 + groups - 1)

    band = router.at[pl.ds(pl.multiple_of(group * columns, columns), columns)]
    spot = band.at[:, pl.ds(pl.multiple_of(me * rows, rows), rows)]
    own_router = pltpu.make_async_copy(part, spot, own_sem.at[1])
    own_router.start()
    router_rows = []
    for j in range(1, n):
        router_rows.append(
            pltpu.make_async_remote_copy(
                src_ref=part, dst_ref=spot, send_sem=rs_send.at[j], recv_sem=rs_recv.at[j],
                device_id=(group, lax.rem(me + j, n)), device_id_type=MESH,
            )
        )
        router_rows[-1].start()

    half, quarter = n // 2, max(n // 4, 1)
    lower = me < half
    outer = jnp.logical_or(me < quarter, me >= n - quarter)
    near = [lax.rem(me + j, half) + jnp.where(lower, 0, half) for j in range(1, half)]
    far = [lax.rem(me + j, half) + jnp.where(lower, half, 0) for j in range(half)]

    def send(e, peer):
        pltpu.make_async_remote_copy(
            src_ref=outbox.at[peer, e], dst_ref=recv.at[me, e],
            send_sem=send_sem.at[peer], recv_sem=recv_sem.at[me],
            device_id=(group, peer), device_id_type=MESH,
        ).start()

    def send_first(e):
        if ORDER == 0:
            for peer in far + near:
                send(e, peer)
        elif ORDER == 1:
            for peer in near + far:
                send(e, peer)
        else:
            @pl.when(outer)
            def _():
                for peer in near:
                    send(e, peer)

            @pl.when(jnp.logical_not(outer))
            def _():
                for peer in far:
                    send(e, peer)

    def send_second(e):
        @pl.when(outer)
        def _():
            for peer in far:
                send(e, peer)

        @pl.when(jnp.logical_not(outer))
        def _():
            for peer in near:
                send(e, peer)

    def step(e, _):
        slot = lax.rem(e, SLOTS)
        for copy in load(e):
            copy.wait()
        for which in range(2):
            merged = wide[slot, which] + narrow[slot, which].astype(jnp.float32)
            turned = merged.astype(jnp.bfloat16).T
            for d in range(n):
                outbox[d, e, which] = turned[d * block:(d + 1) * block]

        @pl.when(e + SLOTS < experts)
        def _():
            for copy in load(e + SLOTS):
                copy.start()

        @pl.when(e > 0)
        def _():
            send_first(e - 1)

        return 0

    lax.fori_loop(0, experts, step, 0)
    send_first(experts - 1)
    if ORDER == 2:
        lax.fori_loop(0, experts, lambda e, c: (send_second(e), c)[1], 0)

    own = pltpu.make_async_copy(outbox.at[me], recv.at[me], own_sem.at[0])
    own.start()

    own_router.wait()
    for copy in router_rows:
        copy.wait()
    router_bands = []
    for j in range(1, groups):
        router_bands.append(
            pltpu.make_async_remote_copy(
                src_ref=band, dst_ref=band, send_sem=re_send.at[j], recv_sem=re_recv.at[j],
                device_id=(lax.rem(group + j, groups), me), device_id_type=MESH,
            )
        )
        router_bands[-1].start()
    for copy in router_bands:
        copy.wait()

    own.wait()
    for j in range(1, n):
        peer = lax.rem(me + j, n)
        pltpu.make_async_copy(outbox.at[peer], outbox.at[peer], send_sem.at[peer]).wait()
        pltpu.make_async_copy(recv.at[peer], recv.at[peer], recv_sem.at[peer]).wait()


def interleave_kernel(n, recv, gate, up):
    rows = recv.shape[-1]
    for d in range(n):
        gate[:, :, d * rows:(d + 1) * rows] = recv[d, :, 0]
        up[:, :, d * rows:(d + 1) * rows] = recv[d, :, 1]


def by_kernel(n, groups, master_gate, second_gate, master_up, second_up, part):
    experts, rows, width = master_gate.shape
    block = width // n
    columns = part.shape[0]
    anywhere = pl.BlockSpec(memory_space=pl.ANY)
    dma = pltpu.SemaphoreType.DMA
    recv, router = pl.pallas_call(
        functools.partial(exchange_kernel, n, groups),
        out_shape=(
            jax.ShapeDtypeStruct((n, experts, 2, block, rows), jnp.bfloat16),
            jax.ShapeDtypeStruct((groups * columns, n * rows), jnp.bfloat16),
        ),
        in_specs=[anywhere] * 5,
        out_specs=(anywhere, anywhere),
        scratch_shapes=[
            pltpu.VMEM((SLOTS, 2, rows, width), jnp.float32),
            pltpu.VMEM((SLOTS, 2, rows, width), jnp.bfloat16),
            pltpu.VMEM((n, experts, 2, block, rows), jnp.bfloat16),
            dma((SLOTS, 4)), dma((n,)), dma((n,)), dma((2,)),
            dma((n,)), dma((n,)), dma((groups,)), dma((groups,)),
        ],
        compiler_params=pltpu.CompilerParams(collective_id=0, has_side_effects=True),
    )(master_gate, second_gate, master_up, second_up, part)
    some = 2 if experts % 2 == 0 else 1
    whole = jax.ShapeDtypeStruct((experts, block, n * rows), jnp.bfloat16)
    gate, up = pl.pallas_call(
        functools.partial(interleave_kernel, n),
        grid=(experts // some,),
        out_shape=(whole, whole),
        in_specs=[pl.BlockSpec((n, some, 2, block, rows), lambda i: (0, i, 0, 0, 0))],
        out_specs=(pl.BlockSpec((some, block, n * rows), lambda i: (i, 0, 0)),) * 2,
    )(recv)
    return gate, up, router.T


def by_collectives(master_gate, second_gate, master_up, second_up, part):
    def moved(master, second):
        narrow = (master + second.astype(jnp.float32)).astype(jnp.bfloat16)
        sent = lax.all_to_all(narrow, "shard", split_axis=2, concat_axis=1, tiled=True)
        return jnp.transpose(sent, (0, 2, 1))

    bands = lax.all_gather(part.T, "shard", axis=0, tiled=True)
    router = lax.all_gather(bands, "expert", axis=1, tiled=True)
    return moved(master_gate, second_gate), moved(master_up, second_up), router


def per_device(n, groups, master_gate, second_gate, master_up, second_up, router_weight, router_gain):
    part = (router_weight * router_gain[:, None]).astype(jnp.bfloat16).T
    experts, rows, width = master_gate.shape
    fits = n >= 4 and n % 4 == 0 and groups > 1 and rows % 128 == 0 and width % (16 * n) == 0
    fits = fits and part.shape[0] % 16 == 0 and experts > SLOTS
    fits = fits and experts * rows * width * 4 + SLOTS * rows * width * 12 < 40 * 2**20
    if fits:
        return by_kernel(n, groups, master_gate, second_gate, master_up, second_up, part)
    return by_collectives(master_gate, second_gate, master_up, second_up, part)


def solution(mesh):
    placed = (
        P("expert", "shard", None),
        P("expert", "shard", None),
        P("expert", "shard", None),
        P("expert", "shard", None),
        P("shard", "expert"),
        P("shard"),
    )
    return jax.shard_map(
        functools.partial(per_device, mesh.shape["shard"], mesh.shape["expert"]),
        mesh=mesh,
        in_specs=placed,
        out_specs=(P("expert", "shard", None), P("expert", "shard", None), P()),
        check_vma=False,
    )
```
